256 devices in a mesh: zero: 16 (over y, x), width: 16 (over z, core).
Axes of the slice: x: 4, y: 4, z: 8, core: 2. Of those that a mesh axis runs over, the one named last changes fastest.
Arguments:
- train_gate: float32 [5120, 13824], P('zero', 'width'), may hold values from -0.125 to 0.125
- drift_gate: float32 [5120, 13824], P('zero', 'width'), may hold values from -0.078125 to 0.078125
- spread_gate: float32 [5120, 13824], P('zero', 'width'), may hold values from -0.078125 to 0.078125
- train_up: float32 [5120, 13824], P('zero', 'width'), may hold values from -0.125 to 0.125
- drift_up: float32 [5120, 13824], P('zero', 'width'), may hold values from -0.078125 to 0.078125
- spread_up: float32 [5120, 13824], P('zero', 'width'), may hold values from -0.078125 to 0.078125
- norm_gain: float32 [5120], P('zero'), may hold values from 0.25 to 1.75
Outputs:
- serving_gate: bfloat16 [5120, 13824], P(None, 'width')
- serving_up: bfloat16 [5120, 13824], P(None, 'width')
- factor_gate: float32 [13824], P('width')
- factor_up: float32 [13824], P('width')
The draws below stay inside these ranges and needn't reach their ends.
All inputs are finite; a program needn't handle non-finite values. Where the reference program divides by a largest or mean magnitude, that divisor is 1e-20 or more.
Results may differ from the reference program's by a relative error of at most 0.001.
Values may be sent and summed in bfloat16 or wider, within the bound.
A program may use at most 192 MiB of HBM per device.

```python
import jax
import jax.numpy as jnp

D_MODEL = 5120
D_INNER = 13824


def spiked(values, key, source, target, blocks, factor):
    def block_of(axis_at):
        return (jnp.arange(values.shape[axis_at]) // (values.shape[axis_at] // blocks)).reshape((-1,) + (1,) * (values.ndim - 1 - axis_at))

    one_side = jax.random.permutation(key, blocks)[block_of(target)]
    second = (block_of(target) + blocks // 2) % blocks
    return jnp.where((block_of(source) == one_side) | (block_of(source) == second), factor * values, values)


def block_scale(key, dims, cuts, least, high):
    gain, own = 1.0, jax.random.fold_in(key, 6)
    for axis_at, blocks in cuts:
        steps = jnp.exp(jax.random.uniform(jax.random.fold_in(own, axis_at), (blocks,), jnp.float32, least / len(cuts), high / len(cuts)))
        gain = gain * jnp.repeat(steps, dims[axis_at] // blocks).reshape([-1 if axis == axis_at else 1 for axis in range(len(dims))])
    return gain


def normal_values(rng, extent, width, bound, cuts=(), kind=jnp.bfloat16):
    result = jax.random.normal(rng, extent, jnp.float32) * width
    if len(cuts) > 0:
        result = block_scale(rng, extent, cuts, -0.22, 0.18) * result
    return jnp.clip(result, min=-bound, max=bound).astype(kind)


def heavy_noise(own_key, dims, deviation, bound, cuts, heavy, held_as=jnp.bfloat16):
    array = deviation * jax.random.normal(own_key, dims, jnp.float32)
    if cuts:
        array = array * block_scale(own_key, dims, cuts, -0.22, 0.18)
    return jnp.clip(spiked(array, jax.random.fold_in(own_key, 3), *heavy), -bound, bound).astype(held_as)


def setup_inputs(seed: int = 0) -> dict:
    arg_keys = jax.random.split(jax.random.key(seed), 8)
    return {
        "train_gate": heavy_noise(arg_keys[0], (D_MODEL, D_INNER), D_MODEL ** -0.5, 0.125, ((0, 16), (1, 16)), (0, 1, 16, 2.0), jnp.float32),
        "drift_gate": normal_values(arg_keys[1], (D_MODEL, D_INNER), D_MODEL ** -0.5, 0.078125, ((0, 16), (1, 16)), jnp.float32),
        "spread_gate": normal_values(arg_keys[2], (D_MODEL, D_INNER), D_MODEL ** -0.5, 0.078125, ((0, 16), (1, 16)), jnp.float32),
        "train_up": heavy_noise(arg_keys[3], (D_MODEL, D_INNER), D_MODEL ** -0.5, 0.125, ((0, 16), (1, 16)), (0, 1, 16, 2.0), jnp.float32),
        "drift_up": normal_values(arg_keys[4], (D_MODEL, D_INNER), D_MODEL ** -0.5, 0.078125, ((0, 16), (1, 16)), jnp.float32),
        "spread_up": normal_values(arg_keys[5], (D_MODEL, D_INNER), D_MODEL ** -0.5, 0.078125, ((0, 16), (1, 16)), jnp.float32),
        "norm_gain": jnp.clip(1.0 + 0.15 * jax.random.normal(arg_keys[6], (D_MODEL,), jnp.float32), 0.25, 1.75),
    }


learn_rate = 0.3
hold_rate = 0.9


def reference(train_gate, drift_gate, spread_gate, train_up, drift_up, spread_up, norm_gain):
    hold_gate = hold_rate * drift_gate + spread_gate
    whole_gate = train_gate - learn_rate * hold_gate
    hold_up = hold_rate * drift_up + spread_up
    whole_up = train_up - learn_rate * hold_up
    whole_gained_gate = whole_gate * norm_gain[:, None]
    whole_gained_up = whole_up * norm_gain[:, None]
    factor_gate = jnp.max(jnp.abs(whole_gained_gate), axis=0)
    serving_gate = (whole_gained_gate / factor_gate).astype(jnp.bfloat16)
    factor_up = jnp.max(jnp.abs(whole_gained_up), axis=0)
    serving_up = (whole_gained_up / factor_up).astype(jnp.bfloat16)
    return serving_gate, serving_up, factor_gate, factor_up
```

```python
import functools

import jax
import jax.numpy as jnp
from jax import lax
from jax.experimental import pallas as pl
from jax.experimental.pallas import tpu as pltpu
from jax.sharding import PartitionSpec as P

learn_rate = 0.3
hold_rate = 0.9

SIDE = 4
GROUP = SIDE * SIDE
ROWS = 320
COLS = 864
LANES = 128
TILES = 7
HALF = 64
PIECES = 4
PIECE = COLS // PIECES
FIRST = 112
SECOND = PIECE - FIRST
PACKED = 2 * PIECE + FIRST
ARRAY_PIECES = GROUP * PIECES

OWN_SLOTS = (("f", 1), ("f", 2), (0, 1), (0, 2))
LATER_SLOTS = (
    ("f", 3), (0, 3), (-1, 1), (1, 1), (2, 1), (-1, 2), (-1, 3), (1, 2), (1, 3), (2, 2), (2, 3),
)
LINKS = (("x", 1), ("x", -1), ("y", 1), ("y", -1))


def sent_in(link, slot):
    axis, sign = link
    block, part = slot
    first = 0 if axis == "x" else 1
    half = first if block == "f" else 1 - first
    lead = 0 if sign == 1 else 1
    piece = 2 * half + (1 - lead if part == 2 else lead)
    along = -sign if part == 3 else 0
    across = 0 if block == "f" else block
    dx, dy = (along, across) if axis == "x" else (across, along)
    return dx % SIDE, dy % SIDE, piece


def received_in(link, slot):
    axis, sign = link
    dx, dy, piece = sent_in(link, slot)
    if axis == "x":
        dx = (dx - sign) % SIDE
    else:
        dy = (dy - sign) % SIDE
    return dx, dy, piece


def kernel(
    train_gate, drift_gate, spread_gate, train_up, drift_up, spread_up, gain,
    out_gate, out_up, factor_gate, factor_up,
    train, drift, spread, whole, turned, gains, gain_columns, factor_columns, land, maxima,
    in_sem, gain_sem, max_send, max_recv, send_sem, recv_sem,
):
    me = lax.axis_index("zero")
    my_x, my_y = lax.rem(me, SIDE), me // SIDE

    def device(dx, dy):
        return lax.rem(my_y + dy, SIDE) * SIDE + lax.rem(my_x + dx, SIDE)

    def peer(step):
        return lax.rem(me + step, GROUP)

    sources = ((train_gate, drift_gate, spread_gate), (train_up, drift_up, spread_up))
    outs = (out_gate, out_up)
    factors = (factor_gate, factor_up)

    gain_copy = pltpu.make_async_copy(gain, gains, gain_sem)
    gain_copy.start()
    loads = []
    for a in range(2):
        for k, (source, target) in enumerate(zip(sources[a], (train, drift, spread))):
            copy = pltpu.make_async_copy(source, target.at[a], in_sem.at[a, k])
            copy.start()
            loads.append(copy)

    barrier = pltpu.get_barrier_semaphore()
    for step in range(1, GROUP):
        pl.semaphore_signal(
            barrier, inc=1, device_id={"zero": peer(step)}, device_id_type=pl.DeviceIdType.MESH
        )

    for a in range(2):
        whole[a, :, (TILES - 1) * LANES :] = jnp.zeros((ROWS, LANES), jnp.float32)

    gain_copy.wait()
    for at in range(0, ROWS, LANES):
        count = min(LANES, ROWS - at)
        row = lax.broadcasted_iota(jnp.int32, (count, count), 0)
        column = lax.broadcasted_iota(jnp.int32, (count, count), 1)
        some = gains[at : at + count].reshape(1, count)
        diagonal = jnp.where(row == column, some, 0.0)
        gain_columns[at : at + count, :] = jnp.broadcast_to(
            jnp.sum(diagonal, axis=1, keepdims=True), (count, LANES)
        )

    def tile(c):
        return slice(c * LANES, min((c + 1) * LANES, COLS))

    def step_and_send(a):
        for k in range(3):
            loads[3 * a + k].wait()

        def stripe(i, tops):
            at = pl.ds(pl.multiple_of(i * 8, 8), 8)
            scale = gain_columns[at, :]
            new = []
            for c in range(TILES):
                hold = hold_rate * drift[a, at, tile(c)] + spread[a, at, tile(c)]
                value = (train[a, at, tile(c)] - learn_rate * hold) * scale[:, : hold.shape[1]]
                whole[a, at, tile(c)] = value
                new.append(jnp.maximum(tops[c], jnp.abs(value)))
            return tuple(new)

        tops = lax.fori_loop(
            0,
            ROWS // 8,
            stripe,
            tuple(jnp.zeros((8, min(LANES, COLS - c * LANES)), jnp.float32) for c in range(TILES)),
            unroll=2,
        )
        maxima[a, 0] = jnp.zeros((8, LANES), jnp.float32)
        for c in range(TILES):
            maxima[a, 0, c : c + 1, : tops[c].shape[1]] = jnp.max(tops[c], axis=0, keepdims=True)
        if a == 0:
            pl.semaphore_wait(barrier, GROUP - 1)
        for step in range(1, GROUP):
            pltpu.make_async_remote_copy(
                src_ref=maxima.at[a, 0],
                dst_ref=maxima.at[a, step],
                send_sem=max_send.at[a],
                recv_sem=max_recv.at[a],
                device_id={"zero": peer(step)},
                device_id_type=pl.DeviceIdType.MESH,
            ).start()

    def piece_at(a, dx, dy, piece):
        return a * ARRAY_PIECES + device(dx, dy) * PIECES + piece

    odd = lax.rem(me, 2)

    def turn(a):
        starts = (odd * HALF, odd * HALF + LANES)
        for c in range(TILES):
            columns = slice(c * LANES, (c + 1) * LANES)
            for k, start in enumerate(starts):
                rows = pl.ds(pl.multiple_of(start, HALF), LANES)
                turned[a, columns, k * LANES : (k + 1) * LANES] = whole[a, rows, columns].T
            rows = pl.ds(pl.multiple_of((1 - odd) * 4 * HALF, HALF), HALF)
            turned[a, columns, 2 * LANES : 2 * LANES + HALF] = whole[a, rows, columns].T

    def round_own(a):
        rest = maxima.at[a, pl.ds(1, GROUP - 1)]
        pltpu.make_async_copy(rest, rest, max_recv.at[a]).wait()
        factor = jnp.max(maxima[a], axis=0)
        factors[a][...] = factor
        upright = factor.T
        for c in range(TILES):
            factor_columns[c * LANES : (c + 1) * LANES, :] = jnp.broadcast_to(
                upright[:, c : c + 1], (LANES, LANES)
            )
        own = a * ARRAY_PIECES + me * PIECES

        def one(piece, carry):
            start = piece * PIECE
            at = pl.ds(pl.multiple_of(start, 8), PIECE)
            divisor = factor_columns[at, :]
            for k in range(2):
                value = turned[a, at, k * LANES : (k + 1) * LANES] / divisor
                land[own + piece, k * PIECE : (k + 1) * PIECE, :] = value.astype(jnp.bfloat16)
            value = turned[a, at, 2 * LANES :] / divisor
            left = lax.broadcasted_iota(jnp.int32, (SECOND, LANES), 1) < HALF
            both = jnp.where(left, value[:SECOND], pltpu.roll(value[FIRST:], HALF, 1))
            land[own + piece, 2 * PIECE : 2 * PIECE + SECOND, :] = both.astype(jnp.bfloat16)
            land[own + piece, 2 * PIECE + SECOND :, :] = value[SECOND:FIRST].astype(jnp.bfloat16)
            return carry

        lax.fori_loop(0, PIECES, one, 0)

    def send(a, link, slot):
        axis, sign = link
        at = piece_at(a, *sent_in(link, slot))
        towards = device(sign % SIDE, 0) if axis == "x" else device(0, sign % SIDE)
        pltpu.make_async_remote_copy(
            src_ref=land.at[at],
            dst_ref=land.at[at],
            send_sem=send_sem.at[LINKS.index(link)],
            recv_sem=recv_sem.at[at],
            device_id={"zero": towards},
            device_id_type=pl.DeviceIdType.MESH,
        ).start()

    arrived = set()

    def await_piece(a, where):
        if (a, where) in arrived or where[:2] == (0, 0):
            return
        arrived.add((a, where))
        at = piece_at(a, *where)
        pltpu.make_async_copy(land.at[at], land.at[at], recv_sem.at[at]).wait()

    def unpack(a, where):
        await_piece(a, where)
        dx, dy, piece = where
        at = piece_at(a, *where)
        source = device(dx, dy)
        right = lax.rem(source, 2)
        base = (source // 2) * 5 * LANES
        full = pl.multiple_of(base + right * 3 * LANES, LANES)
        shared = pl.multiple_of(base + 2 * LANES, LANES)
        start = piece * PIECE
        for k in range(2):
            outs[a][start : start + PIECE, pl.ds(pl.multiple_of(full + k * LANES, LANES), LANES)] = land[
                at, k * PIECE : (k + 1) * PIECE, :
            ]
        for begin, count, place in ((0, FIRST, 0), (FIRST, SECOND, 1)):
            rows = slice(start + begin, start + begin + count)
            value = land[at, 2 * PIECE : 2 * PIECE + count, :].astype(jnp.float32)
            value = pltpu.roll(value, lax.rem(right + place, 2) * HALF, 1)
            lane = lax.broadcasted_iota(jnp.int32, (count, LANES), 1)
            mine = (lane // HALF) == right
            old = outs[a][rows, pl.ds(shared, LANES)].astype(jnp.float32)
            outs[a][rows, pl.ds(shared, LANES)] = jnp.where(mine, value, old).astype(jnp.bfloat16)

    step_and_send(0)
    step_and_send(1)
    for a in range(2):
        turn(a)
        round_own(a)
        for slot in OWN_SLOTS:
            for link in LINKS:
                send(a, link, slot)
    for a in range(2):
        for piece in range(PIECES):
            unpack(a, (0, 0, piece))

    order = [(a, slot) for a in range(2) for slot in OWN_SLOTS]
    done = 0
    for a, slot in ((a, slot) for a in range(2) for slot in LATER_SLOTS):
        for link in LINKS:
            await_piece(a, sent_in(link, slot))
            send(a, link, slot)
        order.append((a, slot))
        while done < len(order) - 3:
            for link in LINKS:
                unpack(order[done][0], received_in(link, order[done][1]))
            done += 1
    for a, slot in order[done:]:
        for link in LINKS:
            unpack(a, received_in(link, slot))

    for a in range(2):
        rest = maxima.at[a, pl.ds(1, GROUP - 1)]
        pltpu.make_async_copy(rest, rest, max_send.at[a]).wait()
    sent = land.at[pl.ds(0, 2 * (len(OWN_SLOTS) + len(LATER_SLOTS)))]
    for k in range(len(LINKS)):
        pltpu.make_async_copy(sent, sent, send_sem.at[k]).wait()


def body(train_gate, drift_gate, spread_gate, train_up, drift_up, spread_up, norm_gain):
    anywhere = pl.BlockSpec(memory_space=pltpu.HBM)
    near = pl.BlockSpec(memory_space=pltpu.VMEM)
    serving_gate, serving_up, factor_gate, factor_up = pl.pallas_call(
        kernel,
        out_shape=(
            pltpu.VMEM((COLS, GROUP * ROWS), jnp.bfloat16),
            pltpu.VMEM((COLS, GROUP * ROWS), jnp.bfloat16),
            pltpu.VMEM((8, LANES), jnp.float32),
            pltpu.VMEM((8, LANES), jnp.float32),
        ),
        in_specs=[anywhere] * 7,
        out_specs=(near,) * 4,
        scratch_shapes=[
            pltpu.VMEM((2, ROWS, COLS), jnp.float32),
            pltpu.VMEM((2, ROWS, COLS), jnp.float32),
            pltpu.VMEM((2, ROWS, COLS), jnp.float32),
            pltpu.VMEM((2, ROWS, TILES * LANES), jnp.float32),
            pltpu.VMEM((2, TILES * LANES, 3 * LANES), jnp.float32),
            pltpu.VMEM((ROWS,), jnp.float32),
            pltpu.VMEM((ROWS, LANES), jnp.float32),
            pltpu.VMEM((TILES * LANES, LANES), jnp.float32),
            pltpu.VMEM((2 * ARRAY_PIECES, PACKED, LANES), jnp.bfloat16),
            pltpu.VMEM((2, GROUP, 8, LANES), jnp.float32),
            pltpu.SemaphoreType.DMA((2, 3)),
            pltpu.SemaphoreType.DMA,
            pltpu.SemaphoreType.DMA((2,)),
            pltpu.SemaphoreType.DMA((2,)),
            pltpu.SemaphoreType.DMA((len(LINKS),)),
            pltpu.SemaphoreType.DMA((2 * ARRAY_PIECES,)),
        ],
        compiler_params=pltpu.CompilerParams(
            collective_id=0, has_side_effects=True, vmem_limit_bytes=45 << 20
        ),
        name="step_and_gather",
    )(train_gate, drift_gate, spread_gate, train_up, drift_up, spread_up, norm_gain)
    return (
        serving_gate.T,
        serving_up.T,
        factor_gate.reshape(-1)[:COLS],
        factor_up.reshape(-1)[:COLS],
    )


def solution(mesh):
    return jax.shard_map(
        body,
        mesh=mesh,
        in_specs=(P("zero", "width"),) * 6 + (P("zero"),),
        out_specs=(P(None, "width"), P(None, "width"), P("width"), P("width")),
        check_vma=False,
    )
```

```python
import functools

import jax
import jax.numpy as jnp
from jax import lax
from jax.experimental import pallas as pl
from jax.experimental.pallas import tpu as pltpu
from jax.sharding import PartitionSpec as P

learn_rate = 0.3
hold_rate = 0.9

SIDE = 4
GROUP = SIDE * SIDE
ROWS = 320
COLS = 864
LANES = 128
TILES = 7
HALF = 64
PIECES = 4
SIZES = ((224, 208, 208, 224), (208, 224, 224, 208))
STARTS = tuple(tuple(sum(sizes[:k]) for k in range(PIECES)) for sizes in SIZES)
LARGEST = max(SIZES[0]) * 5 // 2
ARRAY_PIECES = GROUP * PIECES
OUT_PARTS = 4

OWN_SLOTS = (("f", 1), ("f", 2), (0, 1), (0, 2))
LATER_SLOTS = (
    ("f", 3), (0, 3), (-1, 1), (1, 1), (2, 1), (-1, 2), (-1, 3), (1, 2), (1, 3), (2, 2), (2, 3),
)
LINKS = (("x", 1), ("x", -1), ("y", 1), ("y", -1))
LINK_SLOTS = len(OWN_SLOTS) + len(LATER_SLOTS)


def hops(peer):
    return sum(min(d, SIDE - d) for d in peer)


PEERS = sorted(((dx, dy) for dx in range(SIDE) for dy in range(SIDE)), key=hops)[:0:-1]


def sent_in(link, slot):
    axis, sign = link
    block, part = slot
    first = 0 if axis == "x" else 1
    half = first if block == "f" else 1 - first
    lead = 0 if sign == 1 else 1
    piece = 2 * half + (1 - lead if part == 2 else lead)
    along = -sign if part == 3 else 0
    across = 0 if block == "f" else block
    dx, dy = (along, across) if axis == "x" else (across, along)
    return dx % SIDE, dy % SIDE, piece


def received_in(link, slot):
    axis, sign = link
    dx, dy, piece = sent_in(link, slot)
    if axis == "x":
        dx = (dx - sign) % SIDE
    else:
        dy = (dy - sign) % SIDE
    return dx, dy, piece


def kernel(
    train_gate, drift_gate, spread_gate, train_up, drift_up, spread_up, gain,
    out_gate, out_up, factor_gate, factor_up,
    train, drift, spread, whole, turned, gains, gain_columns, factor_columns, land, maxima,
    in_sem, gain_sem, max_send, max_recv, send_sem, recv_sem,
):
    me = lax.axis_index("zero")
    my_x, my_y = lax.rem(me, SIDE), me // SIDE

    def device(dx, dy):
        return lax.rem(my_y + dy, SIDE) * SIDE + lax.rem(my_x + dx, SIDE)

    sources = ((train_gate, drift_gate, spread_gate), (train_up, drift_up, spread_up))
    outs = (out_gate, out_up)
    factors = (factor_gate, factor_up)

    gain_copy = pltpu.make_async_copy(gain, gains, gain_sem)
    gain_copy.start()
    loads = []
    for a in range(2):
        for k, (source, target) in enumerate(zip(sources[a], (train, drift, spread))):
            loads.append(pltpu.make_async_copy(source, target.at[a], in_sem.at[a, k]))
    for copy in loads[:3]:
        copy.start()

    barrier = pltpu.get_barrier_semaphore()
    for peer in PEERS:
        pl.semaphore_signal(
            barrier,
            inc=1,
            device_id={"zero": device(*peer)},
            device_id_type=pl.DeviceIdType.MESH,
        )

    for a in range(2):
        whole[a, :, (TILES - 1) * LANES :] = jnp.zeros((ROWS, LANES), jnp.float32)

    gain_copy.wait()
    for at in range(0, ROWS, LANES):
        count = min(LANES, ROWS - at)
        row = lax.broadcasted_iota(jnp.int32, (count, count), 0)
        column = lax.broadcasted_iota(jnp.int32, (count, count), 1)
        some = gains[at : at + count].reshape(1, count)
        diagonal = jnp.where(row == column, some, 0.0)
        gain_columns[at : at + count, :] = jnp.broadcast_to(
            jnp.sum(diagonal, axis=1, keepdims=True), (count, LANES)
        )

    def tile(c):
        return slice(c * LANES, min((c + 1) * LANES, COLS))

    def step_and_send(a):
        for k in range(3):
            loads[3 * a + k].wait()
        if a == 0:
            for copy in loads[3:]:
                copy.start()

        def stripe(i, tops):
            at = pl.ds(pl.multiple_of(i * 8, 8), 8)
            scale = gain_columns[at, :]
            new = []
            for c in range(TILES):
                hold = hold_rate * drift[a, at, tile(c)] + spread[a, at, tile(c)]
                value = (train[a, at, tile(c)] - learn_rate * hold) * scale[:, : hold.shape[1]]
                whole[a, at, tile(c)] = value
                new.append(jnp.maximum(tops[c], jnp.abs(value)))
            return tuple(new)

        tops = lax.fori_loop(
            0,
            ROWS // 8,
            stripe,
            tuple(jnp.zeros((8, min(LANES, COLS - c * LANES)), jnp.float32) for c in range(TILES)),
            unroll=2,
        )
        maxima[a, 0] = jnp.zeros((8, LANES), jnp.float32)
        for c in range(TILES):
            maxima[a, 0, c : c + 1, : tops[c].shape[1]] = jnp.max(tops[c], axis=0, keepdims=True)
        if a == 0:
            pl.semaphore_wait(barrier, GROUP - 1)
        for dx, dy in PEERS:
            pltpu.make_async_remote_copy(
                src_ref=maxima.at[a, 0],
                dst_ref=maxima.at[a, dy * SIDE + dx],
                send_sem=max_send.at[a],
                recv_sem=max_recv.at[a],
                device_id={"zero": device(dx, dy)},
                device_id_type=pl.DeviceIdType.MESH,
            ).start()

    def piece_at(a, dx, dy, piece):
        return a * ARRAY_PIECES + device(dx, dy) * PIECES + piece

    odd = lax.rem(me, 2)

    def turn(a):
        starts = (odd * HALF, odd * HALF + LANES)
        for c in range(TILES):
            columns = slice(c * LANES, (c + 1) * LANES)
            for k, start in enumerate(starts):
                rows = pl.ds(pl.multiple_of(start, HALF), LANES)
                turned[a, columns, k * LANES : (k + 1) * LANES] = whole[a, rows, columns].T
            rows = pl.ds(pl.multiple_of((1 - odd) * 4 * HALF, HALF), HALF)
            turned[a, columns, 2 * LANES : 2 * LANES + HALF] = whole[a, rows, columns].T

    def take_factor(a):
        rest = maxima.at[a, pl.ds(1, GROUP - 1)]
        pltpu.make_async_copy(rest, rest, max_recv.at[a]).wait()
        factor = jnp.max(maxima[a], axis=0)
        factors[a][...] = factor
        upright = factor.T
        for c in range(TILES):
            factor_columns[c * LANES : (c + 1) * LANES, :] = jnp.broadcast_to(
                upright[:, c : c + 1], (LANES, LANES)
            )

    def round_piece(a, piece):
        at = piece_at(a, 0, 0, piece)
        size, start = SIZES[a][piece], STARTS[a][piece]
        columns = slice(start, start + size)
        divisor = factor_columns[columns, :]
        for k in range(2):
            value = turned[a, columns, k * LANES : (k + 1) * LANES] / divisor
            land[at, k * size : (k + 1) * size, :] = value.astype(jnp.bfloat16)
        value = turned[a, columns, 2 * LANES :] / divisor
        left = lax.broadcasted_iota(jnp.int32, (size // 2, LANES), 1) < HALF
        both = jnp.where(left, value[: size // 2], pltpu.roll(value[size // 2 :], HALF, 1))
        land[at, 2 * size : size * 5 // 2, :] = both.astype(jnp.bfloat16)

    def send(a, link, slot):
        axis, sign = link
        where = sent_in(link, slot)
        towards = device(sign % SIDE, 0) if axis == "x" else device(0, sign % SIDE)
        copy = pltpu.make_async_remote_copy(
            src_ref=held(a, where),
            dst_ref=held(a, where),
            send_sem=send_sem.at[len(sends)],
            recv_sem=recv_sem.at[piece_at(a, *where)],
            device_id={"zero": towards},
            device_id_type=pl.DeviceIdType.MESH,
        )
        copy.start()
        sends.append(copy)

    def held(a, where):
        return land.at[piece_at(a, *where), pl.ds(0, SIZES[a][where[2]] * 5 // 2)]

    sends = []
    arrived = set()

    def await_piece(a, where):
        if (a, where) in arrived or where[:2] == (0, 0):
            return
        arrived.add((a, where))
        ref = held(a, where)
        pltpu.make_async_copy(ref, ref, recv_sem.at[piece_at(a, *where)]).wait()

    def unpack(a, where):
        await_piece(a, where)
        dx, dy, piece = where
        at = piece_at(a, *where)
        source = device(dx, dy)
        right = lax.rem(source, 2)
        base = (source // 2) * 5 * LANES
        full = pl.multiple_of(base + right * 3 * LANES, LANES)
        shared = pl.multiple_of(base + 2 * LANES, LANES)
        size, start = SIZES[a][piece], STARTS[a][piece]
        count = size // 2
        for k in range(2):
            outs[a][start : start + size, pl.ds(pl.multiple_of(full + k * LANES, LANES), LANES)] = land[
                at, k * size : (k + 1) * size, :
            ]
        for place in range(2):
            rows = slice(start + place * count, start + (place + 1) * count)
            value = land[at, 2 * size : 2 * size + count, :].astype(jnp.float32)
            value = pltpu.roll(value, lax.rem(right + place, 2) * HALF, 1)
            lane = lax.broadcasted_iota(jnp.int32, (count, LANES), 1)
            mine = (lane // HALF) == right
            old = outs[a][rows, pl.ds(shared, LANES)].astype(jnp.float32)
            outs[a][rows, pl.ds(shared, LANES)] = jnp.where(mine, value, old).astype(jnp.bfloat16)

    step_and_send(0)
    step_and_send(1)
    for a in range(2):
        turn(a)
        take_factor(a)
        for piece in (0, 2, 1, 3):
            round_piece(a, piece)
            for link in LINKS:
                if sent_in(link, OWN_SLOTS[0])[2] == piece:
                    send(a, link, OWN_SLOTS[0])
        for slot in OWN_SLOTS[1:]:
            for link in LINKS:
                send(a, link, slot)
    for a in range(2):
        for piece in range(PIECES):
            unpack(a, (0, 0, piece))

    order = [(a, slot) for a in range(2) for slot in OWN_SLOTS]
    done = 0
    for a, slot in ((a, slot) for a in range(2) for slot in LATER_SLOTS):
        for link in LINKS:
            await_piece(a, sent_in(link, slot))
            send(a, link, slot)
        order.append((a, slot))
        while done < len(order) - 3:
            for link in LINKS:
                unpack(order[done][0], received_in(link, order[done][1]))
            done += 1
    for a, slot in order[done:]:
        for link in LINKS:
            unpack(a, received_in(link, slot))

    for a in range(2):
        rest = maxima.at[a, pl.ds(1, GROUP - 1)]
        pltpu.make_async_copy(rest, rest, max_send.at[a]).wait()
    for copy in sends:
        copy.wait_send()


def copy_out(gate, up, factor_gate, factor_up, to_gate, to_up, to_factor_gate, to_factor_up, sems):
    copies = []
    for source, target in ((factor_gate, to_factor_gate), (factor_up, to_factor_up)):
        copies.append(pltpu.make_async_copy(source, target, sems.at[len(copies)]))
    for part in range(OUT_PARTS):
        rows = pl.ds(part * (COLS // OUT_PARTS), COLS // OUT_PARTS)
        for source, target in ((gate, to_gate), (up, to_up)):
            copies.append(
                pltpu.make_async_copy(source.at[rows], target.at[rows], sems.at[len(copies)])
            )
    for copy in copies:
        copy.start()
    for copy in copies:
        copy.wait()


def body(train_gate, drift_gate, spread_gate, train_up, drift_up, spread_up, norm_gain):
    anywhere = pl.BlockSpec(memory_space=pltpu.HBM)
    near = pl.BlockSpec(memory_space=pltpu.VMEM)
    results = pl.pallas_call(
        kernel,
        out_shape=(
            pltpu.VMEM((COLS, GROUP * ROWS), jnp.bfloat16),
            pltpu.VMEM((COLS, GROUP * ROWS), jnp.bfloat16),
            pltpu.VMEM((8, LANES), jnp.float32),
            pltpu.VMEM((8, LANES), jnp.float32),
        ),
        in_specs=[anywhere] * 7,
        out_specs=(near,) * 4,
        scratch_shapes=[
            pltpu.VMEM((2, ROWS, COLS), jnp.float32),
            pltpu.VMEM((2, ROWS, COLS), jnp.float32),
            pltpu.VMEM((2, ROWS, COLS), jnp.float32),
            pltpu.VMEM((2, ROWS, TILES * LANES), jnp.float32),
            pltpu.VMEM((2, TILES * LANES, 3 * LANES), jnp.float32),
            pltpu.VMEM((ROWS,), jnp.float32),
            pltpu.VMEM((ROWS, LANES), jnp.float32),
            pltpu.VMEM((TILES * LANES, LANES), jnp.float32),
            pltpu.VMEM((2 * ARRAY_PIECES, LARGEST, LANES), jnp.bfloat16),
            pltpu.VMEM((2, GROUP, 8, LANES), jnp.float32),
            pltpu.SemaphoreType.DMA((2, 3)),
            pltpu.SemaphoreType.DMA,
            pltpu.SemaphoreType.DMA((2,)),
            pltpu.SemaphoreType.DMA((2,)),
            pltpu.SemaphoreType.DMA((2 * len(LINKS) * LINK_SLOTS,)),
            pltpu.SemaphoreType.DMA((2 * ARRAY_PIECES,)),
        ],
        compiler_params=pltpu.CompilerParams(
            collective_id=0, has_side_effects=True, vmem_limit_bytes=45 << 20
        ),
        name="step_and_gather",
    )(train_gate, drift_gate, spread_gate, train_up, drift_up, spread_up, norm_gain)
    far = pl.BlockSpec(memory_space=pltpu.HBM)
    serving_gate, serving_up, factor_gate, factor_up = pl.pallas_call(
        copy_out,
        out_shape=(
            jax.ShapeDtypeStruct((COLS, GROUP * ROWS), jnp.bfloat16),
            jax.ShapeDtypeStruct((COLS, GROUP * ROWS), jnp.bfloat16),
            jax.ShapeDtypeStruct((8, LANES), jnp.float32),
            jax.ShapeDtypeStruct((8, LANES), jnp.float32),
        ),
        in_specs=[pl.BlockSpec(memory_space=pl.ANY)] * 4,
        out_specs=(far,) * 4,
        scratch_shapes=[pltpu.SemaphoreType.DMA((2 + 2 * OUT_PARTS,))],
        compiler_params=pltpu.CompilerParams(vmem_limit_bytes=1 << 20),
        name="copy_out",
    )(*results)
    return (
        serving_gate.T,
        serving_up.T,
        factor_gate.reshape(-1)[:COLS],
        factor_up.reshape(-1)[:COLS],
    )


def solution(mesh):
    return jax.shard_map(
        body,
        mesh=mesh,
        in_specs=(P("zero", "width"),) * 6 + (P("zero"),),
        out_specs=(P(None, "width"), P(None, "width"), P("width"), P("width")),
        check_vma=False,
    )
```

```python
import functools

import jax
import jax.numpy as jnp
from jax import lax
from jax.experimental import pallas as pl
from jax.experimental.pallas import tpu as pltpu
from jax.sharding import PartitionSpec as P

learn_rate = 0.3
hold_rate = 0.9

SIDE = 4
GROUP = SIDE * SIDE
ROWS = 320
COLS = 864
LANES = 128
TILES = 7
HALF = 64
PIECES = 4
SIZES = ((224, 208, 208, 224), (208, 224, 224, 208))
STARTS = tuple(tuple(sum(sizes[:k]) for k in range(PIECES)) for sizes in SIZES)
LARGEST = max(SIZES[0]) * 5 // 2
ARRAY_PIECES = GROUP * PIECES
OUT_PARTS = 4
EARLY = 1

OWN_SLOTS = (("f", 1), ("f", 2), (0, 1), (0, 2))
LATER_SLOTS = (
    ("f", 3), (0, 3), (-1, 1), (1, 1), (2, 1), (-1, 2), (-1, 3), (1, 2), (1, 3), (2, 2), (2, 3),
)
LINKS = (("x", 1), ("x", -1), ("y", 1), ("y", -1))
LINK_SLOTS = len(OWN_SLOTS) + len(LATER_SLOTS)


def hops(peer):
    return sum(min(d, SIDE - d) for d in peer)


PEERS = sorted(((dx, dy) for dx in range(SIDE) for dy in range(SIDE)), key=hops)[:0:-1]


def sent_in(link, slot):
    axis, sign = link
    block, part = slot
    first = 0 if axis == "x" else 1
    half = first if block == "f" else 1 - first
    lead = 0 if sign == 1 else 1
    piece = 2 * half + (1 - lead if part == 2 else lead)
    along = -sign if part == 3 else 0
    across = 0 if block == "f" else block
    dx, dy = (along, across) if axis == "x" else (across, along)
    return dx % SIDE, dy % SIDE, piece


def received_in(link, slot):
    axis, sign = link
    dx, dy, piece = sent_in(link, slot)
    if axis == "x":
        dx = (dx - sign) % SIDE
    else:
        dy = (dy - sign) % SIDE
    return dx, dy, piece


def kernel(
    train_gate, drift_gate, spread_gate, train_up, drift_up, spread_up, gain,
    out_gate, out_up, factor_gate, factor_up,
    train, drift, spread, whole, turned, early, gains, gain_columns, factor_columns, land, maxima,
    in_sem, gain_sem, max_send, max_recv, send_sem, recv_sem, early_sem,
):
    me = lax.axis_index("zero")
    my_x, my_y = lax.rem(me, SIDE), me // SIDE

    def device(dx, dy):
        return lax.rem(my_y + dy, SIDE) * SIDE + lax.rem(my_x + dx, SIDE)

    sources = ((train_gate, drift_gate, spread_gate), (train_up, drift_up, spread_up))
    outs = (out_gate, out_up)
    factors = (factor_gate, factor_up)

    gain_copy = pltpu.make_async_copy(gain, gains, gain_sem)
    gain_copy.start()
    loads = []
    for a in range(2):
        for k, (source, target) in enumerate(zip(sources[a], (train, drift, spread))):
            loads.append(pltpu.make_async_copy(source, target.at[a], in_sem.at[a, k]))
    for copy in loads[:3]:
        copy.start()

    barrier = pltpu.get_barrier_semaphore()
    for peer in PEERS:
        pl.semaphore_signal(
            barrier,
            inc=1,
            device_id={"zero": device(*peer)},
            device_id_type=pl.DeviceIdType.MESH,
        )

    gain_copy.wait()
    for at in range(0, ROWS, LANES):
        count = min(LANES, ROWS - at)
        row = lax.broadcasted_iota(jnp.int32, (count, count), 0)
        column = lax.broadcasted_iota(jnp.int32, (count, count), 1)
        some = gains[at : at + count].reshape(1, count)
        diagonal = jnp.where(row == column, some, 0.0)
        gain_columns[at : at + count, :] = jnp.broadcast_to(
            jnp.sum(diagonal, axis=1, keepdims=True), (count, LANES)
        )

    def tile(c):
        return slice(c * LANES, min((c + 1) * LANES, COLS))

    def step(a):
        for k in range(3):
            loads[3 * a + k].wait()
        if a == 0:
            for copy in loads[3:]:
                copy.start()

        def stripe(i, tops):
            at = pl.ds(pl.multiple_of(i * 8, 8), 8)
            scale = gain_columns[at, :]
            new = []
            for c in range(TILES):
                hold = hold_rate * drift[a, at, tile(c)] + spread[a, at, tile(c)]
                value = (train[a, at, tile(c)] - learn_rate * hold) * scale[:, : hold.shape[1]]
                whole[a, at, tile(c)] = value
                new.append(jnp.maximum(tops[c], jnp.abs(value)))
            return tuple(new)

        tops = lax.fori_loop(
            0,
            ROWS // 8,
            stripe,
            tuple(jnp.zeros((8, min(LANES, COLS - c * LANES)), jnp.float32) for c in range(TILES)),
            unroll=2,
        )
        maxima[a, 0] = jnp.zeros((8, LANES), jnp.float32)
        for c in range(TILES):
            maxima[a, 0, c : c + 1, : tops[c].shape[1]] = jnp.max(tops[c], axis=0, keepdims=True)

    def send_maxima(a):
        for dx, dy in PEERS:
            pltpu.make_async_remote_copy(
                src_ref=maxima.at[a, 0],
                dst_ref=maxima.at[a, dy * SIDE + dx],
                send_sem=max_send.at[a],
                recv_sem=max_recv.at[a],
                device_id={"zero": device(dx, dy)},
                device_id_type=pl.DeviceIdType.MESH,
            ).start()

    def piece_at(a, dx, dy, piece):
        return a * ARRAY_PIECES + device(dx, dy) * PIECES + piece

    odd = lax.rem(me, 2)

    def turn(a, tiles):
        starts = (odd * HALF, odd * HALF + LANES)
        for c in tiles:
            columns = slice(c * LANES, (c + 1) * LANES)
            values = []
            for begin in starts:
                rows = pl.ds(pl.multiple_of(begin, HALF), LANES)
                values.append(whole[a, rows, columns].T)
            rows = pl.ds(pl.multiple_of((1 - odd) * 4 * HALF, HALF), HALF)
            half = whole[a, rows, columns]
            values.append(jnp.concatenate([half, half], axis=0).T)
            for piece in range(PIECES):
                size, start = SIZES[a][piece], STARTS[a][piece]
                for place in range(2):
                    first = start + place * (size // 2)
                    low = max(first, c * LANES)
                    high = min(first + size // 2, (c + 1) * LANES)
                    if low >= high:
                        continue
                    taken = slice(low - c * LANES, high - c * LANES)
                    for k in range(2):
                        at = k * size + low - start
                        turned[a, piece, at : at + high - low, :] = values[k][taken]
                    at = 2 * size + low - first
                    lanes = slice(place * HALF, (place + 1) * HALF)
                    turned[a, piece, at : at + high - low, lanes] = values[2][taken, lanes]

    def take_factor(a):
        rest = maxima.at[a, pl.ds(1, GROUP - 1)]
        pltpu.make_async_copy(rest, rest, max_recv.at[a]).wait()
        factor = jnp.max(maxima[a], axis=0)
        factors[a][...] = factor
        upright = factor.T
        for c in range(TILES):
            factor_columns[a, c * LANES : (c + 1) * LANES, :] = jnp.broadcast_to(
                upright[:, c : c + 1], (LANES, LANES)
            )

    def round_blocks(a, source, where, blocks):
        at, piece = piece_at(a, *where), where[2]
        size, start = SIZES[a][piece], STARTS[a][piece]
        divisor = factor_columns[a, start : start + size, :]
        for k in blocks:
            value = source[k * size : (k + 1) * size, :] / divisor
            land[at, k * size : (k + 1) * size, :] = value.astype(jnp.bfloat16)

    def round_piece(a, source, where):
        round_blocks(a, source, where, range(2))
        at, piece = piece_at(a, *where), where[2]
        size, start = SIZES[a][piece], STARTS[a][piece]
        divisor = factor_columns[a, start : start + size, :]
        left = lax.broadcasted_iota(jnp.int32, (size // 2, LANES), 1) < HALF
        value = source[2 * size : size * 5 // 2, :]
        value = value / jnp.where(left, divisor[: size // 2], divisor[size // 2 :])
        land[at, 2 * size : size * 5 // 2, :] = value.astype(jnp.bfloat16)

    def start_send(link, source, target, arrival):
        axis, sign = link
        towards = device(sign % SIDE, 0) if axis == "x" else device(0, sign % SIDE)
        copy = pltpu.make_async_remote_copy(
            src_ref=source,
            dst_ref=target,
            send_sem=send_sem.at[len(sends)],
            recv_sem=arrival,
            device_id={"zero": towards},
            device_id_type=pl.DeviceIdType.MESH,
        )
        copy.start()
        sends.append(copy)

    def send(a, link, slot):
        where = sent_in(link, slot)
        start_send(link, held(a, where), held(a, where), recv_sem.at[piece_at(a, *where)])

    def early_ref(link, piece):
        return early.at[LINKS.index(link), pl.ds(0, EARLY * SIZES[0][piece])]

    def rest_of(where):
        size = SIZES[0][where[2]]
        return land.at[piece_at(0, *where), pl.ds(EARLY * size, size * 5 // 2 - EARLY * size)]

    def send_rest(link):
        where = sent_in(link, OWN_SLOTS[0])
        start_send(link, rest_of(where), rest_of(where), recv_sem.at[piece_at(0, *where)])

    def send_early(link):
        piece = sent_in(link, OWN_SLOTS[0])[2]
        source = turned.at[0, piece, pl.ds(0, EARLY * SIZES[0][piece])]
        start_send(link, source, early_ref(link, piece), early_sem.at[LINKS.index(link)])

    def held(a, where):
        return land.at[piece_at(a, *where), pl.ds(0, SIZES[a][where[2]] * 5 // 2)]

    sends = []
    arrived = set()

    def await_piece(a, where):
        if (a, where) in arrived or where[:2] == (0, 0):
            return
        arrived.add((a, where))
        for k, link in enumerate(LINKS):
            if (a, where) == (0, received_in(link, OWN_SLOTS[0])):
                ref = early_ref(link, where[2])
                pltpu.make_async_copy(ref, ref, early_sem.at[k]).wait()
                round_blocks(a, early.at[k], where, range(EARLY))
                ref = rest_of(where)
                pltpu.make_async_copy(ref, ref, recv_sem.at[piece_at(a, *where)]).wait()
                return
        ref = held(a, where)
        pltpu.make_async_copy(ref, ref, recv_sem.at[piece_at(a, *where)]).wait()

    def unpack(a, where):
        await_piece(a, where)
        dx, dy, piece = where
        at = piece_at(a, *where)
        source = device(dx, dy)
        right = lax.rem(source, 2)
        base = (source // 2) * 5 * LANES
        full = pl.multiple_of(base + right * 3 * LANES, LANES)
        shared = pl.multiple_of(base + 2 * LANES, LANES)
        size, start = SIZES[a][piece], STARTS[a][piece]
        count = size // 2
        for k in range(2):
            outs[a][start : start + size, pl.ds(pl.multiple_of(full + k * LANES, LANES), LANES)] = land[
                at, k * size : (k + 1) * size, :
            ]
        for place in range(2):
            rows = slice(start + place * count, start + (place + 1) * count)
            value = land[at, 2 * size : 2 * size + count, :].astype(jnp.float32)
            value = pltpu.roll(value, lax.rem(right + place, 2) * HALF, 1)
            lane = lax.broadcasted_iota(jnp.int32, (count, LANES), 1)
            mine = (lane // HALF) == right
            old = outs[a][rows, pl.ds(shared, LANES)].astype(jnp.float32)
            outs[a][rows, pl.ds(shared, LANES)] = jnp.where(mine, value, old).astype(jnp.bfloat16)

    step(0)
    turn(0, range(4))
    pl.semaphore_wait(barrier, GROUP - 1)
    send_maxima(0)
    for link in LINKS[:2]:
        send_early(link)
    turn(0, range(4, TILES))
    for link in LINKS[2:]:
        send_early(link)
    step(1)
    send_maxima(1)
    turn(1, range(TILES))
    for a in range(2):
        take_factor(a)
        for piece in range(PIECES):
            round_piece(a, turned.at[a, piece], (0, 0, piece))
        if a == 0:
            for link in LINKS:
                send_rest(link)
        for slot in OWN_SLOTS[1 - a :]:
            for link in LINKS:
                send(a, link, slot)
    for a in range(2):
        for piece in range(PIECES):
            unpack(a, (0, 0, piece))

    order = [(a, slot) for a in range(2) for slot in OWN_SLOTS]
    done = 0
    for a, slot in ((a, slot) for a in range(2) for slot in LATER_SLOTS):
        for link in LINKS:
            await_piece(a, sent_in(link, slot))
            send(a, link, slot)
        order.append((a, slot))
        while done < len(order) - 3:
            for link in LINKS:
                unpack(order[done][0], received_in(link, order[done][1]))
            done += 1
    for a, slot in order[done:]:
        for link in LINKS:
            unpack(a, received_in(link, slot))

    for a in range(2):
        rest = maxima.at[a, pl.ds(1, GROUP - 1)]
        pltpu.make_async_copy(rest, rest, max_send.at[a]).wait()
    for copy in sends:
        copy.wait_send()


def copy_out(gate, up, factor_gate, factor_up, to_gate, to_up, to_factor_gate, to_factor_up, sems):
    copies = []
    for source, target in ((factor_gate, to_factor_gate), (factor_up, to_factor_up)):
        copies.append(pltpu.make_async_copy(source, target, sems.at[len(copies)]))
    for part in range(OUT_PARTS):
        rows = pl.ds(part * (COLS // OUT_PARTS), COLS // OUT_PARTS)
        for source, target in ((gate, to_gate), (up, to_up)):
            copies.append(
                pltpu.make_async_copy(source.at[rows], target.at[rows], sems.at[len(copies)])
            )
    for copy in copies:
        copy.start()
    for copy in copies:
        copy.wait()


def body(train_gate, drift_gate, spread_gate, train_up, drift_up, spread_up, norm_gain):
    anywhere = pl.BlockSpec(memory_space=pltpu.HBM)
    near = pl.BlockSpec(memory_space=pltpu.VMEM)
    results = pl.pallas_call(
        kernel,
        out_shape=(
            pltpu.VMEM((COLS, GROUP * ROWS), jnp.bfloat16),
            pltpu.VMEM((COLS, GROUP * ROWS), jnp.bfloat16),
            pltpu.VMEM((8, LANES), jnp.float32),
            pltpu.VMEM((8, LANES), jnp.float32),
        ),
        in_specs=[anywhere] * 7,
        out_specs=(near,) * 4,
        scratch_shapes=[
            pltpu.VMEM((2, ROWS, COLS), jnp.float32),
            pltpu.VMEM((2, ROWS, COLS), jnp.float32),
            pltpu.VMEM((2, ROWS, COLS), jnp.float32),
            pltpu.VMEM((2, ROWS, TILES * LANES), jnp.float32),
            pltpu.VMEM((2, PIECES, LARGEST, LANES), jnp.float32),
            pltpu.VMEM((len(LINKS), EARLY * max(SIZES[0]), LANES), jnp.float32),
            pltpu.VMEM((ROWS,), jnp.float32),
            pltpu.VMEM((ROWS, LANES), jnp.float32),
            pltpu.VMEM((2, TILES * LANES, LANES), jnp.float32),
            pltpu.VMEM((2 * ARRAY_PIECES, LARGEST, LANES), jnp.bfloat16),
            pltpu.VMEM((2, GROUP, 8, LANES), jnp.float32),
            pltpu.SemaphoreType.DMA((2, 3)),
            pltpu.SemaphoreType.DMA,
            pltpu.SemaphoreType.DMA((2,)),
            pltpu.SemaphoreType.DMA((2,)),
            pltpu.SemaphoreType.DMA(((2 * LINK_SLOTS + 1) * len(LINKS),)),
            pltpu.SemaphoreType.DMA((2 * ARRAY_PIECES,)),
            pltpu.SemaphoreType.DMA((len(LINKS),)),
        ],
        compiler_params=pltpu.CompilerParams(
            collective_id=0, has_side_effects=True, vmem_limit_bytes=45 << 20
        ),
        name="step_and_gather",
    )(train_gate, drift_gate, spread_gate, train_up, drift_up, spread_up, norm_gain)
    far = pl.BlockSpec(memory_space=pltpu.HBM)
    serving_gate, serving_up, factor_gate, factor_up = pl.pallas_call(
        copy_out,
        out_shape=(
            jax.ShapeDtypeStruct((COLS, GROUP * ROWS), jnp.bfloat16),
            jax.ShapeDtypeStruct((COLS, GROUP * ROWS), jnp.bfloat16),
            jax.ShapeDtypeStruct((8, LANES), jnp.float32),
            jax.ShapeDtypeStruct((8, LANES), jnp.float32),
        ),
        in_specs=[pl.BlockSpec(memory_space=pl.ANY)] * 4,
        out_specs=(far,) * 4,
        scratch_shapes=[pltpu.SemaphoreType.DMA((2 + 2 * OUT_PARTS,))],
        compiler_params=pltpu.CompilerParams(vmem_limit_bytes=1 << 20),
        name="copy_out",
    )(*results)
    return (
        serving_gate.T,
        serving_up.T,
        factor_gate.reshape(-1)[:COLS],
        factor_up.reshape(-1)[:COLS],
    )


def solution(mesh):
    return jax.shard_map(
        body,
        mesh=mesh,
        in_specs=(P("zero", "width"),) * 6 + (P("zero"),),
        out_specs=(P(None, "width"), P(None, "width"), P("width"), P("width")),
        check_vma=False,
    )
```

```python
import functools

import jax
import jax.numpy as jnp
from jax import lax
from jax.experimental import pallas as pl
from jax.experimental.pallas import tpu as pltpu
from jax.sharding import PartitionSpec as P

learn_rate = 0.3
hold_rate = 0.9

SIDE = 4
GROUP = SIDE * SIDE
ROWS = 320
COLS = 864
LANES = 128
TILES = 7
HALF = 64
PIECES = 4
SIZES = ((224, 208, 208, 224), (208, 224, 224, 208))
STARTS = tuple(tuple(sum(sizes[:k]) for k in range(PIECES)) for sizes in SIZES)
LARGEST = max(SIZES[0]) * 5 // 2
ARRAY_PIECES = GROUP * PIECES
OUT_PARTS = 4
EARLY = 1

OWN_SLOTS = (("f", 1), ("f", 2), (0, 1), (0, 2))
LATER_SLOTS = (
    ("f", 3), (0, 3), (-1, 1), (1, 1), (2, 1), (-1, 2), (-1, 3), (1, 2), (1, 3), (2, 2), (2, 3),
)
LINKS = (("x", 1), ("x", -1), ("y", 1), ("y", -1))
LINK_SLOTS = len(OWN_SLOTS) + len(LATER_SLOTS)


def hops(peer):
    return sum(min(d, SIDE - d) for d in peer)


PEERS = sorted(((dx, dy) for dx in range(SIDE) for dy in range(SIDE)), key=hops)[:0:-1]


def sent_in(link, slot):
    axis, sign = link
    block, part = slot
    first = 0 if axis == "x" else 1
    half = first if block == "f" else 1 - first
    lead = 0 if sign == 1 else 1
    piece = 2 * half + (1 - lead if part == 2 else lead)
    along = -sign if part == 3 else 0
    across = 0 if block == "f" else block
    dx, dy = (along, across) if axis == "x" else (across, along)
    return dx % SIDE, dy % SIDE, piece


def received_in(link, slot):
    axis, sign = link
    dx, dy, piece = sent_in(link, slot)
    if axis == "x":
        dx = (dx - sign) % SIDE
    else:
        dy = (dy - sign) % SIDE
    return dx, dy, piece


def kernel(
    train_gate, drift_gate, spread_gate, train_up, drift_up, spread_up, gain,
    out_gate, out_up, factor_gate, factor_up,
    train, drift, spread, whole, turned, early, gains, gain_columns, factor_columns, land, maxima,
    in_sem, gain_sem, max_send, max_recv, send_sem, recv_sem, early_sem,
):
    me = lax.axis_index("zero")
    my_x, my_y = lax.rem(me, SIDE), me // SIDE

    def device(dx, dy):
        return lax.rem(my_y + dy, SIDE) * SIDE + lax.rem(my_x + dx, SIDE)

    sources = ((train_gate, drift_gate, spread_gate), (train_up, drift_up, spread_up))
    outs = (out_gate, out_up)
    factors = (factor_gate, factor_up)

    gain_copy = pltpu.make_async_copy(gain, gains, gain_sem)
    gain_copy.start()
    loads = []
    for a in range(2):
        for k, (source, target) in enumerate(zip(sources[a], (train, drift, spread))):
            loads.append(pltpu.make_async_copy(source, target.at[a], in_sem.at[a, k]))
    for copy in loads[:3]:
        copy.start()

    barrier = pltpu.get_barrier_semaphore()
    for peer in PEERS:
        pl.semaphore_signal(
            barrier,
            inc=1,
            device_id={"zero": device(*peer)},
            device_id_type=pl.DeviceIdType.MESH,
        )

    gain_copy.wait()
    for at in range(0, ROWS, LANES):
        count = min(LANES, ROWS - at)
        row = lax.broadcasted_iota(jnp.int32, (count, count), 0)
        column = lax.broadcasted_iota(jnp.int32, (count, count), 1)
        some = gains[at : at + count].reshape(1, count)
        diagonal = jnp.where(row == column, some, 0.0)
        gain_columns[at : at + count, :] = jnp.broadcast_to(
            jnp.sum(diagonal, axis=1, keepdims=True), (count, LANES)
        )

    def tile(c):
        return slice(c * LANES, min((c + 1) * LANES, COLS))

    def step(a):
        for k in range(3):
            loads[3 * a + k].wait()
        if a == 0:
            for copy in loads[3:]:
                copy.start()

        def stripe(i, tops):
            at = pl.ds(pl.multiple_of(i * 8, 8), 8)
            scale = gain_columns[at, :]
            new = []
            for c in range(TILES):
                hold = hold_rate * drift[a, at, tile(c)] + spread[a, at, tile(c)]
                value = (train[a, at, tile(c)] - learn_rate * hold) * scale[:, : hold.shape[1]]
                whole[a, at, tile(c)] = value
                new.append(jnp.maximum(tops[c], jnp.abs(value)))
            return tuple(new)

        tops = lax.fori_loop(
            0,
            ROWS // 8,
            stripe,
            tuple(jnp.zeros((8, min(LANES, COLS - c * LANES)), jnp.float32) for c in range(TILES)),
            unroll=2,
        )
        maxima[a, 0] = jnp.zeros((8, LANES), jnp.float32)
        for c in range(TILES):
            maxima[a, 0, c : c + 1, : tops[c].shape[1]] = jnp.max(tops[c], axis=0, keepdims=True)

    def send_maxima(a):
        for dx, dy in PEERS:
            pltpu.make_async_remote_copy(
                src_ref=maxima.at[a, 0],
                dst_ref=maxima.at[a, dy * SIDE + dx],
                send_sem=max_send.at[a],
                recv_sem=max_recv.at[a],
                device_id={"zero": device(dx, dy)},
                device_id_type=pl.DeviceIdType.MESH,
            ).start()

    def piece_at(a, dx, dy, piece):
        return a * ARRAY_PIECES + device(dx, dy) * PIECES + piece

    odd = lax.rem(me, 2)

    def turn(a, tiles):
        starts = (odd * HALF, odd * HALF + LANES)
        for c in tiles:
            columns = slice(c * LANES, (c + 1) * LANES)
            values = []
            for begin in starts:
                rows = pl.ds(pl.multiple_of(begin, HALF), LANES)
                values.append(whole[a, rows, columns].T)
            rows = pl.ds(pl.multiple_of((1 - odd) * 4 * HALF, HALF), HALF)
            half = whole[a, rows, columns]
            values.append(jnp.concatenate([half, half], axis=0).T)
            for piece in range(PIECES):
                size, start = SIZES[a][piece], STARTS[a][piece]
                for place in range(2):
                    first = start + place * (size // 2)
                    low = max(first, c * LANES)
                    high = min(first + size // 2, (c + 1) * LANES)
                    if low >= high:
                        continue
                    taken = slice(low - c * LANES, high - c * LANES)
                    for k in range(2):
                        at = k * size + low - start
                        turned[a, piece, at : at + high - low, :] = values[k][taken]
                    at = 2 * size + low - first
                    lanes = slice(place * HALF, (place + 1) * HALF)
                    turned[a, piece, at : at + high - low, lanes] = values[2][taken, lanes]

    def take_factor(a):
        rest = maxima.at[a, pl.ds(1, GROUP - 1)]
        pltpu.make_async_copy(rest, rest, max_recv.at[a]).wait()
        factor = jnp.max(maxima[a], axis=0)
        factors[a][...] = factor
        upright = factor.T
        for c in range(TILES):
            factor_columns[a, c * LANES : (c + 1) * LANES, :] = jnp.broadcast_to(
                upright[:, c : c + 1], (LANES, LANES)
            )

    def round_blocks(a, source, where, blocks):
        at, piece = piece_at(a, *where), where[2]
        size, start = SIZES[a][piece], STARTS[a][piece]
        divisor = factor_columns[a, start : start + size, :]
        for k in blocks:
            value = source[k * size : (k + 1) * size, :] / divisor
            land[at, k * size : (k + 1) * size, :] = value.astype(jnp.bfloat16)

    def round_shared(a, source, where):
        at, piece = piece_at(a, *where), where[2]
        size, start = SIZES[a][piece], STARTS[a][piece]
        divisor = factor_columns[a, start : start + size, :]
        left = lax.broadcasted_iota(jnp.int32, (size // 2, LANES), 1) < HALF
        value = source[2 * size : size * 5 // 2, :]
        value = value / jnp.where(left, divisor[: size // 2], divisor[size // 2 :])
        land[at, 2 * size : size * 5 // 2, :] = value.astype(jnp.bfloat16)

    def start_send(link, source, target, arrival):
        axis, sign = link
        towards = device(sign % SIDE, 0) if axis == "x" else device(0, sign % SIDE)
        copy = pltpu.make_async_remote_copy(
            src_ref=source,
            dst_ref=target,
            send_sem=send_sem.at[len(sends)],
            recv_sem=arrival,
            device_id={"zero": towards},
            device_id_type=pl.DeviceIdType.MESH,
        )
        copy.start()
        sends.append(copy)

    def send(a, link, slot):
        where = sent_in(link, slot)
        start_send(link, held(a, where), held(a, where), recv_sem.at[piece_at(a, *where)])

    def early_ref(link, piece):
        return early.at[LINKS.index(link), pl.ds(0, EARLY * SIZES[0][piece])]

    def rest_of(where):
        size = SIZES[0][where[2]]
        return land.at[piece_at(0, *where), pl.ds(EARLY * size, size * 5 // 2 - EARLY * size)]

    def send_rest(link):
        where = sent_in(link, OWN_SLOTS[0])
        start_send(link, rest_of(where), rest_of(where), recv_sem.at[piece_at(0, *where)])

    def send_early(link):
        piece = sent_in(link, OWN_SLOTS[0])[2]
        source = turned.at[0, piece, pl.ds(0, EARLY * SIZES[0][piece])]
        start_send(link, source, early_ref(link, piece), early_sem.at[LINKS.index(link)])

    def held(a, where):
        return land.at[piece_at(a, *where), pl.ds(0, SIZES[a][where[2]] * 5 // 2)]

    sends = []
    arrived = set()

    def await_piece(a, where):
        if (a, where) in arrived or where[:2] == (0, 0):
            return
        arrived.add((a, where))
        for k, link in enumerate(LINKS):
            if (a, where) == (0, received_in(link, OWN_SLOTS[0])):
                ref = early_ref(link, where[2])
                pltpu.make_async_copy(ref, ref, early_sem.at[k]).wait()
                round_blocks(a, early.at[k], where, range(EARLY))
                ref = rest_of(where)
                pltpu.make_async_copy(ref, ref, recv_sem.at[piece_at(a, *where)]).wait()
                return
        ref = held(a, where)
        pltpu.make_async_copy(ref, ref, recv_sem.at[piece_at(a, *where)]).wait()

    def unpack(a, where):
        await_piece(a, where)
        dx, dy, piece = where
        at = piece_at(a, *where)
        source = device(dx, dy)
        right = lax.rem(source, 2)
        base = (source // 2) * 5 * LANES
        full = pl.multiple_of(base + right * 3 * LANES, LANES)
        shared = pl.multiple_of(base + 2 * LANES, LANES)
        size, start = SIZES[a][piece], STARTS[a][piece]
        count = size // 2
        for k in range(2):
            outs[a][start : start + size, pl.ds(pl.multiple_of(full + k * LANES, LANES), LANES)] = land[
                at, k * size : (k + 1) * size, :
            ]
        for place in range(2):
            rows = slice(start + place * count, start + (place + 1) * count)
            value = land[at, 2 * size : 2 * size + count, :].astype(jnp.float32)
            value = pltpu.roll(value, lax.rem(right + place, 2) * HALF, 1)
            lane = lax.broadcasted_iota(jnp.int32, (count, LANES), 1)
            mine = (lane // HALF) == right
            old = outs[a][rows, pl.ds(shared, LANES)].astype(jnp.float32)
            outs[a][rows, pl.ds(shared, LANES)] = jnp.where(mine, value, old).astype(jnp.bfloat16)

    step(0)
    turn(0, range(4))
    pl.semaphore_wait(barrier, GROUP - 1)
    send_maxima(0)
    for link in LINKS[:2]:
        send_early(link)
    turn(0, range(4, TILES))
    for link in LINKS[2:]:
        send_early(link)
    step(1)
    send_maxima(1)
    turn(1, range(TILES))
    for a in range(2):
        take_factor(a)
        late = EARLY if a == 0 else 0
        for link in LINKS:
            piece = sent_in(link, OWN_SLOTS[0])[2]
            round_blocks(a, turned.at[a, piece], (0, 0, piece), range(late, 2))
            round_shared(a, turned.at[a, piece], (0, 0, piece))
            if a == 0:
                send_rest(link)
        for piece in range(PIECES):
            round_blocks(a, turned.at[a, piece], (0, 0, piece), range(late))
        for slot in OWN_SLOTS[1 - a :]:
            for link in LINKS:
                send(a, link, slot)
    for a in range(2):
        for piece in range(PIECES):
            unpack(a, (0, 0, piece))

    order = [(a, slot) for a in range(2) for slot in OWN_SLOTS]
    done = waited = 0
    for a, slot in ((a, slot) for a in range(2) for slot in LATER_SLOTS):
        for link in LINKS:
            await_piece(a, sent_in(link, slot))
            send(a, link, slot)
        order.append((a, slot))
        while done < len(order) - 3:
            for link in LINKS:
                unpack(order[done][0], received_in(link, order[done][1]))
            done += 1
        while waited < len(sends) - 5 * len(LINKS):
            sends[waited].wait_send()
            waited += 1
    for a, slot in order[done:]:
        for link in LINKS:
            unpack(a, received_in(link, slot))

    for a in range(2):
        rest = maxima.at[a, pl.ds(1, GROUP - 1)]
        pltpu.make_async_copy(rest, rest, max_send.at[a]).wait()
    for copy in sends[waited:]:
        copy.wait_send()


def copy_out(gate, up, factor_gate, factor_up, to_gate, to_up, to_factor_gate, to_factor_up, sems):
    copies = []
    for source, target in ((factor_gate, to_factor_gate), (factor_up, to_factor_up)):
        copies.append(pltpu.make_async_copy(source, target, sems.at[len(copies)]))
    for part in range(OUT_PARTS):
        rows = pl.ds(part * (COLS // OUT_PARTS), COLS // OUT_PARTS)
        for source, target in ((gate, to_gate), (up, to_up)):
            copies.append(
                pltpu.make_async_copy(source.at[rows], target.at[rows], sems.at[len(copies)])
            )
    for copy in copies:
        copy.start()
    for copy in copies:
        copy.wait()


def body(train_gate, drift_gate, spread_gate, train_up, drift_up, spread_up, norm_gain):
    anywhere = pl.BlockSpec(memory_space=pltpu.HBM)
    near = pl.BlockSpec(memory_space=pltpu.VMEM)
    results = pl.pallas_call(
        kernel,
        out_shape=(
            pltpu.VMEM((COLS, GROUP * ROWS), jnp.bfloat16),
            pltpu.VMEM((COLS, GROUP * ROWS), jnp.bfloat16),
            pltpu.VMEM((8, LANES), jnp.float32),
            pltpu.VMEM((8, LANES), jnp.float32),
        ),
        in_specs=[anywhere] * 7,
        out_specs=(near,) * 4,
        scratch_shapes=[
            pltpu.VMEM((2, ROWS, COLS), jnp.float32),
            pltpu.VMEM((2, ROWS, COLS), jnp.float32),
            pltpu.VMEM((2, ROWS, COLS), jnp.float32),
            pltpu.VMEM((2, ROWS, TILES * LANES), jnp.float32),
            pltpu.VMEM((2, PIECES, LARGEST, LANES), jnp.float32),
            pltpu.VMEM((len(LINKS), EARLY * max(SIZES[0]), LANES), jnp.float32),
            pltpu.VMEM((ROWS,), jnp.float32),
            pltpu.VMEM((ROWS, LANES), jnp.float32),
            pltpu.VMEM((2, TILES * LANES, LANES), jnp.float32),
            pltpu.VMEM((2 * ARRAY_PIECES, LARGEST, LANES), jnp.bfloat16),
            pltpu.VMEM((2, GROUP, 8, LANES), jnp.float32),
            pltpu.SemaphoreType.DMA((2, 3)),
            pltpu.SemaphoreType.DMA,
            pltpu.SemaphoreType.DMA((2,)),
            pltpu.SemaphoreType.DMA((2,)),
            pltpu.SemaphoreType.DMA(((2 * LINK_SLOTS + 1) * len(LINKS),)),
            pltpu.SemaphoreType.DMA((2 * ARRAY_PIECES,)),
            pltpu.SemaphoreType.DMA((len(LINKS),)),
        ],
        compiler_params=pltpu.CompilerParams(
            collective_id=0, has_side_effects=True, vmem_limit_bytes=45 << 20
        ),
        name="step_and_gather",
    )(train_gate, drift_gate, spread_gate, train_up, drift_up, spread_up, norm_gain)
    far = pl.BlockSpec(memory_space=pltpu.HBM)
    serving_gate, serving_up, factor_gate, factor_up = pl.pallas_call(
        copy_out,
        out_shape=(
            jax.ShapeDtypeStruct((COLS, GROUP * ROWS), jnp.bfloat16),
            jax.ShapeDtypeStruct((COLS, GROUP * ROWS), jnp.bfloat16),
            jax.ShapeDtypeStruct((8, LANES), jnp.float32),
            jax.ShapeDtypeStruct((8, LANES), jnp.float32),
        ),
        in_specs=[pl.BlockSpec(memory_space=pl.ANY)] * 4,
        out_specs=(far,) * 4,
        scratch_shapes=[pltpu.SemaphoreType.DMA((2 + 2 * OUT_PARTS,))],
        compiler_params=pltpu.CompilerParams(vmem_limit_bytes=1 << 20),
        name="copy_out",
    )(*results)
    return (
        serving_gate.T,
        serving_up.T,
        factor_gate.reshape(-1)[:COLS],
        factor_up.reshape(-1)[:COLS],
    )


def solution(mesh):
    return jax.shard_map(
        body,
        mesh=mesh,
        in_specs=(P("zero", "width"),) * 6 + (P("zero"),),
        out_specs=(P(None, "width"), P(None, "width"), P("width"), P("width")),
        check_vma=False,
    )
```

```python
import functools

import jax
import jax.numpy as jnp
from jax import lax
from jax.experimental import pallas as pl
from jax.experimental.pallas import tpu as pltpu
from jax.sharding import PartitionSpec as P

learn_rate = 0.3
hold_rate = 0.9

SIDE = 4
GROUP = SIDE * SIDE
ROWS = 320
COLS = 864
LANES = 128
TILES = 7
HALF = 64
PIECES = 4
SIZES = ((224, 208, 208, 224), (208, 224, 224, 208))
STARTS = tuple(tuple(sum(sizes[:k]) for k in range(PIECES)) for sizes in SIZES)
LARGEST = max(SIZES[0]) * 5 // 2
ARRAY_PIECES = GROUP * PIECES
OUT_PARTS = 4
EARLY = 1

OWN_SLOTS = (("f", 1), ("f", 2), (0, 1), (0, 2))
LATER_SLOTS = (
    ("f", 3), (0, 3), (-1, 1), (1, 1), (2, 1), (-1, 2), (-1, 3), (1, 2), (1, 3), (2, 2), (2, 3),
)
LINKS = (("x", 1), ("x", -1), ("y", 1), ("y", -1))
LINK_SLOTS = len(OWN_SLOTS) + len(LATER_SLOTS)


def hops(peer):
    return sum(min(d, SIDE - d) for d in peer)


PEERS = sorted(((dx, dy) for dx in range(SIDE) for dy in range(SIDE)), key=hops)[:0:-1]


def sent_in(link, slot):
    axis, sign = link
    block, part = slot
    first = 0 if axis == "x" else 1
    half = first if block == "f" else 1 - first
    lead = 0 if sign == 1 else 1
    piece = 2 * half + (1 - lead if part == 2 else lead)
    along = -sign if part == 3 else 0
    across = 0 if block == "f" else block
    dx, dy = (along, across) if axis == "x" else (across, along)
    return dx % SIDE, dy % SIDE, piece


def received_in(link, slot):
    axis, sign = link
    dx, dy, piece = sent_in(link, slot)
    if axis == "x":
        dx = (dx - sign) % SIDE
    else:
        dy = (dy - sign) % SIDE
    return dx, dy, piece


def kernel(
    train_gate, drift_gate, spread_gate, train_up, drift_up, spread_up, gain,
    out_gate, out_up, factor_gate, factor_up,
    train, drift, spread, whole, turned, early, gains, gain_columns, factor_columns, land, maxima,
    in_sem, gain_sem, max_send, max_recv, send_sem, recv_sem, early_sem,
):
    me = lax.axis_index("zero")
    my_x, my_y = lax.rem(me, SIDE), me // SIDE

    def device(dx, dy):
        return lax.rem(my_y + dy, SIDE) * SIDE + lax.rem(my_x + dx, SIDE)

    sources = ((train_gate, drift_gate, spread_gate), (train_up, drift_up, spread_up))
    outs = (out_gate, out_up)
    factors = (factor_gate, factor_up)

    gain_copy = pltpu.make_async_copy(gain, gains, gain_sem)
    gain_copy.start()
    loads = []
    for a in range(2):
        for k, (source, target) in enumerate(zip(sources[a], (train, drift, spread))):
            loads.append(pltpu.make_async_copy(source, target.at[a], in_sem.at[a, k]))
    for copy in loads[:3]:
        copy.start()

    barrier = pltpu.get_barrier_semaphore()
    for peer in PEERS:
        pl.semaphore_signal(
            barrier,
            inc=1,
            device_id={"zero": device(*peer)},
            device_id_type=pl.DeviceIdType.MESH,
        )

    gain_copy.wait()
    for at in range(0, ROWS, LANES):
        count = min(LANES, ROWS - at)
        row = lax.broadcasted_iota(jnp.int32, (count, count), 0)
        column = lax.broadcasted_iota(jnp.int32, (count, count), 1)
        some = gains[at : at + count].reshape(1, count)
        diagonal = jnp.where(row == column, some, 0.0)
        gain_columns[at : at + count, :] = jnp.broadcast_to(
            jnp.sum(diagonal, axis=1, keepdims=True), (count, LANES)
        )

    def tile(c):
        return slice(c * LANES, min((c + 1) * LANES, COLS))

    def step(a):
        for k in range(3):
            loads[3 * a + k].wait()
        if a == 0:
            for copy in loads[3:]:
                copy.start()

        def stripe(i, tops):
            at = pl.ds(pl.multiple_of(i * 8, 8), 8)
            scale = gain_columns[at, :]
            new = []
            for c in range(TILES):
                hold = hold_rate * drift[a, at, tile(c)] + spread[a, at, tile(c)]
                value = (train[a, at, tile(c)] - learn_rate * hold) * scale[:, : hold.shape[1]]
                whole[a, at, tile(c)] = value
                new.append(jnp.maximum(tops[c], jnp.abs(value)))
            return tuple(new)

        tops = lax.fori_loop(
            0,
            ROWS // 8,
            stripe,
            tuple(jnp.zeros((8, min(LANES, COLS - c * LANES)), jnp.float32) for c in range(TILES)),
            unroll=4,
        )
        maxima[a, 0] = jnp.zeros((8, LANES), jnp.float32)
        for c in range(TILES):
            maxima[a, 0, c : c + 1, : tops[c].shape[1]] = jnp.max(tops[c], axis=0, keepdims=True)

    def send_maxima(a):
        for dx, dy in PEERS:
            pltpu.make_async_remote_copy(
                src_ref=maxima.at[a, 0],
                dst_ref=maxima.at[a, dy * SIDE + dx],
                send_sem=max_send.at[a],
                recv_sem=max_recv.at[a],
                device_id={"zero": device(dx, dy)},
                device_id_type=pl.DeviceIdType.MESH,
            ).start()

    def piece_at(a, dx, dy, piece):
        return a * ARRAY_PIECES + device(dx, dy) * PIECES + piece

    odd = lax.rem(me, 2)

    def turn(a, tiles):
        starts = (odd * HALF, odd * HALF + LANES)
        for c in tiles:
            columns = slice(c * LANES, (c + 1) * LANES)
            values = []
            for begin in starts:
                rows = pl.ds(pl.multiple_of(begin, HALF), LANES)
                values.append(whole[a, rows, columns].T)
            rows = pl.ds(pl.multiple_of((1 - odd) * 4 * HALF, HALF), HALF)
            half = whole[a, rows, columns]
            values.append(jnp.concatenate([half, half], axis=0).T)
            for piece in range(PIECES):
                size, start = SIZES[a][piece], STARTS[a][piece]
                for place in range(2):
                    first = start + place * (size // 2)
                    low = max(first, c * LANES)
                    high = min(first + size // 2, (c + 1) * LANES)
                    if low >= high:
                        continue
                    taken = slice(low - c * LANES, high - c * LANES)
                    for k in range(2):
                        at = k * size + low - start
                        turned[a, piece, at : at + high - low, :] = values[k][taken]
                    at = 2 * size + low - first
                    lanes = slice(place * HALF, (place + 1) * HALF)
                    turned[a, piece, at : at + high - low, lanes] = values[2][taken, lanes]

    def take_factor(a):
        rest = maxima.at[a, pl.ds(1, GROUP - 1)]
        pltpu.make_async_copy(rest, rest, max_recv.at[a]).wait()
        factor = jnp.max(maxima[a], axis=0)
        factors[a][...] = factor
        upright = factor.T
        for c in range(TILES):
            factor_columns[a, c * LANES : (c + 1) * LANES, :] = jnp.broadcast_to(
                upright[:, c : c + 1], (LANES, LANES)
            )

    def round_blocks(a, source, where, blocks):
        at, piece = piece_at(a, *where), where[2]
        size, start = SIZES[a][piece], STARTS[a][piece]
        divisor = factor_columns[a, start : start + size, :]
        for k in blocks:
            value = source[k * size : (k + 1) * size, :] / divisor
            land[at, k * size : (k + 1) * size, :] = value.astype(jnp.bfloat16)

    def round_shared(a, source, where):
        at, piece = piece_at(a, *where), where[2]
        size, start = SIZES[a][piece], STARTS[a][piece]
        divisor = factor_columns[a, start : start + size, :]
        left = lax.broadcasted_iota(jnp.int32, (size // 2, LANES), 1) < HALF
        value = source[2 * size : size * 5 // 2, :]
        value = value / jnp.where(left, divisor[: size // 2], divisor[size // 2 :])
        land[at, 2 * size : size * 5 // 2, :] = value.astype(jnp.bfloat16)

    def start_send(link, source, target, arrival):
        axis, sign = link
        towards = device(sign % SIDE, 0) if axis == "x" else device(0, sign % SIDE)
        copy = pltpu.make_async_remote_copy(
            src_ref=source,
            dst_ref=target,
            send_sem=send_sem.at[len(sends)],
            recv_sem=arrival,
            device_id={"zero": towards},
            device_id_type=pl.DeviceIdType.MESH,
        )
        copy.start()
        sends.append(copy)

    def send(a, link, slot):
        where = sent_in(link, slot)
        start_send(link, held(a, where), held(a, where), recv_sem.at[piece_at(a, *where)])

    def early_ref(link, piece):
        return early.at[LINKS.index(link), pl.ds(0, EARLY * SIZES[0][piece])]

    def rest_of(where):
        size = SIZES[0][where[2]]
        return land.at[piece_at(0, *where), pl.ds(EARLY * size, size * 5 // 2 - EARLY * size)]

    def send_rest(link):
        where = sent_in(link, OWN_SLOTS[0])
        start_send(link, rest_of(where), rest_of(where), recv_sem.at[piece_at(0, *where)])

    def send_early(link):
        piece = sent_in(link, OWN_SLOTS[0])[2]
        source = turned.at[0, piece, pl.ds(0, EARLY * SIZES[0][piece])]
        start_send(link, source, early_ref(link, piece), early_sem.at[LINKS.index(link)])

    def held(a, where):
        return land.at[piece_at(a, *where), pl.ds(0, SIZES[a][where[2]] * 5 // 2)]

    sends = []
    arrived = set()

    def await_piece(a, where):
        if (a, where) in arrived or where[:2] == (0, 0):
            return
        arrived.add((a, where))
        for k, link in enumerate(LINKS):
            if (a, where) == (0, received_in(link, OWN_SLOTS[0])):
                ref = early_ref(link, where[2])
                pltpu.make_async_copy(ref, ref, early_sem.at[k]).wait()
                round_blocks(a, early.at[k], where, range(EARLY))
                ref = rest_of(where)
                pltpu.make_async_copy(ref, ref, recv_sem.at[piece_at(a, *where)]).wait()
                return
        ref = held(a, where)
        pltpu.make_async_copy(ref, ref, recv_sem.at[piece_at(a, *where)]).wait()

    def unpack(a, where):
        await_piece(a, where)
        dx, dy, piece = where
        at = piece_at(a, *where)
        source = device(dx, dy)
        right = lax.rem(source, 2)
        base = (source // 2) * 5 * LANES
        full = pl.multiple_of(base + right * 3 * LANES, LANES)
        shared = pl.multiple_of(base + 2 * LANES, LANES)
        size, start = SIZES[a][piece], STARTS[a][piece]
        count = size // 2
        for k in range(2):
            outs[a][start : start + size, pl.ds(pl.multiple_of(full + k * LANES, LANES), LANES)] = land[
                at, k * size : (k + 1) * size, :
            ]
        for place in range(2):
            rows = slice(start + place * count, start + (place + 1) * count)
            value = land[at, 2 * size : 2 * size + count, :].astype(jnp.float32)
            value = pltpu.roll(value, lax.rem(right + place, 2) * HALF, 1)
            lane = lax.broadcasted_iota(jnp.int32, (count, LANES), 1)
            mine = (lane // HALF) == right
            old = outs[a][rows, pl.ds(shared, LANES)].astype(jnp.float32)
            outs[a][rows, pl.ds(shared, LANES)] = jnp.where(mine, value, old).astype(jnp.bfloat16)

    step(0)
    turn(0, range(4))
    pl.semaphore_wait(barrier, GROUP - 1)
    send_maxima(0)
    for link in LINKS[:2]:
        send_early(link)
    turn(0, range(4, TILES))
    for link in LINKS[2:]:
        send_early(link)
    step(1)
    send_maxima(1)
    turn(1, range(TILES))
    for a in range(2):
        take_factor(a)
        late = EARLY if a == 0 else 0
        for link in LINKS:
            piece = sent_in(link, OWN_SLOTS[0])[2]
            round_blocks(a, turned.at[a, piece], (0, 0, piece), range(late, 2))
            round_shared(a, turned.at[a, piece], (0, 0, piece))
            if a == 0:
                send_rest(link)
        for piece in range(PIECES):
            round_blocks(a, turned.at[a, piece], (0, 0, piece), range(late))
        for slot in OWN_SLOTS[1 - a :]:
            for link in LINKS:
                send(a, link, slot)
    for a in range(2):
        for piece in range(PIECES):
            unpack(a, (0, 0, piece))

    order = [(a, slot) for a in range(2) for slot in OWN_SLOTS]
    done = waited = 0
    for a, slot in ((a, slot) for a in range(2) for slot in LATER_SLOTS):
        for link in LINKS:
            await_piece(a, sent_in(link, slot))
            send(a, link, slot)
        order.append((a, slot))
        while done < len(order) - 3:
            for link in LINKS:
                unpack(order[done][0], received_in(link, order[done][1]))
            done += 1
        while waited < len(sends) - 5 * len(LINKS):
            sends[waited].wait_send()
            waited += 1
    for a, slot in order[done:]:
        for link in LINKS:
            unpack(a, received_in(link, slot))

    for a in range(2):
        rest = maxima.at[a, pl.ds(1, GROUP - 1)]
        pltpu.make_async_copy(rest, rest, max_send.at[a]).wait()
    for copy in sends[waited:]:
        copy.wait_send()


def copy_out(gate, up, factor_gate, factor_up, to_gate, to_up, to_factor_gate, to_factor_up, sems):
    copies = []
    for source, target in ((factor_gate, to_factor_gate), (factor_up, to_factor_up)):
        copies.append(pltpu.make_async_copy(source, target, sems.at[len(copies)]))
    for part in range(OUT_PARTS):
        rows = pl.ds(part * (COLS // OUT_PARTS), COLS // OUT_PARTS)
        for source, target in ((gate, to_gate), (up, to_up)):
            copies.append(
                pltpu.make_async_copy(source.at[rows], target.at[rows], sems.at[len(copies)])
            )
    for copy in copies:
        copy.start()
    for copy in copies:
        copy.wait()


def body(train_gate, drift_gate, spread_gate, train_up, drift_up, spread_up, norm_gain):
    anywhere = pl.BlockSpec(memory_space=pltpu.HBM)
    near = pl.BlockSpec(memory_space=pltpu.VMEM)
    results = pl.pallas_call(
        kernel,
        out_shape=(
            pltpu.VMEM((COLS, GROUP * ROWS), jnp.bfloat16),
            pltpu.VMEM((COLS, GROUP * ROWS), jnp.bfloat16),
            pltpu.VMEM((8, LANES), jnp.float32),
            pltpu.VMEM((8, LANES), jnp.float32),
        ),
        in_specs=[anywhere] * 7,
        out_specs=(near,) * 4,
        scratch_shapes=[
            pltpu.VMEM((2, ROWS, COLS), jnp.float32),
            pltpu.VMEM((2, ROWS, COLS), jnp.float32),
            pltpu.VMEM((2, ROWS, COLS), jnp.float32),
            pltpu.VMEM((2, ROWS, TILES * LANES), jnp.float32),
            pltpu.VMEM((2, PIECES, LARGEST, LANES), jnp.float32),
            pltpu.VMEM((len(LINKS), EARLY * max(SIZES[0]), LANES), jnp.float32),
            pltpu.VMEM((ROWS,), jnp.float32),
            pltpu.VMEM((ROWS, LANES), jnp.float32),
            pltpu.VMEM((2, TILES * LANES, LANES), jnp.float32),
            pltpu.VMEM((2 * ARRAY_PIECES, LARGEST, LANES), jnp.bfloat16),
            pltpu.VMEM((2, GROUP, 8, LANES), jnp.float32),
            pltpu.SemaphoreType.DMA((2, 3)),
            pltpu.SemaphoreType.DMA,
            pltpu.SemaphoreType.DMA((2,)),
            pltpu.SemaphoreType.DMA((2,)),
            pltpu.SemaphoreType.DMA(((2 * LINK_SLOTS + 1) * len(LINKS),)),
            pltpu.SemaphoreType.DMA((2 * ARRAY_PIECES,)),
            pltpu.SemaphoreType.DMA((len(LINKS),)),
        ],
        compiler_params=pltpu.CompilerParams(
            collective_id=0, has_side_effects=True, vmem_limit_bytes=45 << 20
        ),
        name="step_and_gather",
    )(train_gate, drift_gate, spread_gate, train_up, drift_up, spread_up, norm_gain)
    far = pl.BlockSpec(memory_space=pltpu.HBM)
    serving_gate, serving_up, factor_gate, factor_up = pl.pallas_call(
        copy_out,
        out_shape=(
            jax.ShapeDtypeStruct((COLS, GROUP * ROWS), jnp.bfloat16),
            jax.ShapeDtypeStruct((COLS, GROUP * ROWS), jnp.bfloat16),
            jax.ShapeDtypeStruct((8, LANES), jnp.float32),
            jax.ShapeDtypeStruct((8, LANES), jnp.float32),
        ),
        in_specs=[pl.BlockSpec(memory_space=pl.ANY)] * 4,
        out_specs=(far,) * 4,
        scratch_shapes=[pltpu.SemaphoreType.DMA((2 + 2 * OUT_PARTS,))],
        compiler_params=pltpu.CompilerParams(vmem_limit_bytes=1 << 20),
        name="copy_out",
    )(*results)
    return (
        serving_gate.T,
        serving_up.T,
        factor_gate.reshape(-1)[:COLS],
        factor_up.reshape(-1)[:COLS],
    )


def solution(mesh):
    return jax.shard_map(
        body,
        mesh=mesh,
        in_specs=(P("zero", "width"),) * 6 + (P("zero"),),
        out_specs=(P(None, "width"), P(None, "width"), P("width"), P("width")),
        check_vma=False,
    )
```
